32 devices in a mesh: row: 4 (over y, x), col: 8 (over z, core).
Axes of the slice: x: 2, y: 2, z: 4, core: 2. Of those that a mesh axis runs over, the one named last changes fastest.
Arguments:
- activations: float32 [2048, 4096], P('row', 'col')
- plan: int32 [3, 8], P(None, 'col'), may hold values 0 or 1
Outputs:
- rotated: float32 [2048, 4096], P('row', 'col')
- vectors: float32 [4096, 4096], P('row', 'col')
- spread: float32 [4096], P('col')
The draws below stay inside these ranges and needn't reach their ends.
All inputs are finite; a program needn't handle non-finite values. No bound on the sum of `plan` on one device may be relied on, other than what follows from the above.
Results may differ from the reference program's by a relative error of at most 0.0001.
Values sent between devices are 32-bit elements; how exact they have to be, the bound alone decides.
No kernel may reach another device: no remote copies, remote signals or barrier semaphores. Data moves between devices by JAX's collectives and lax.ppermute only.
A program may use at most 64 MiB of HBM per device.

```python
import jax
import jax.numpy as jnp
from jax import lax

P_SIZE = 256
ROUNDS = 3
POLAR_STEPS = 3
PAIRS = 8
N = 4096
M = 2048


def draw_activations(key, part):
    keys = jax.random.split(jax.random.fold_in(key, 17), 4)
    noise = jax.random.normal(keys[0], (M, N), jnp.float32)
    left_factor = jax.random.normal(keys[1], (M, 8), jnp.float32)
    right_factor = jax.random.normal(keys[2], (8, N), jnp.float32)
    col_scale = jnp.exp(jax.random.uniform(keys[3], (N,), jnp.float32, 0.0, 2.302585))
    shared = jnp.dot(left_factor, right_factor) * (0.6 / 2.828427)
    values = (noise + shared) * col_scale[None, :]
    return values.astype(jnp.float32)


def place_ends(entries, key, smallest, top_value):
    dims = entries.shape
    spot = [jax.random.randint(jax.random.fold_in(key, axis), (), 0, dims[axis]) for axis in range(len(dims))]
    entries = entries.at[tuple(spot)].set(smallest)
    longest = dims.index(max(dims))
    spot[longest] = (spot[longest] + 1) % dims[longest]
    return entries.at[tuple(spot)].set(top_value)


def setup_inputs(seed: int = 0) -> dict:
    key_list = jax.random.split(jax.random.key(seed), 3)
    return {
        "activations": draw_activations(jax.random.fold_in(key_list[2], 71), 0),
        "plan": place_ends((jax.random.randint(key_list[1], (ROUNDS, PAIRS), 0, 2) < 1).astype(jnp.int32), jax.random.fold_in(key_list[1], 1), 0, 1),
    }


HIGH = lax.Precision.HIGHEST

def rotation(pair_gram):
    half_width = pair_gram.shape[0] // 2
    diagonal = jnp.diagonal(pair_gram) + 1e-06
    root_diag = jnp.sqrt(diagonal)
    coupling = pair_gram[:half_width, half_width:] / (root_diag[:half_width, None] * root_diag[None, half_width:])
    strength = jnp.sqrt(jnp.sum(coupling * coupling))
    scaled = coupling / (1.0 + strength)
    zeros_block = jnp.zeros((half_width, half_width), jnp.float32)
    generator = jnp.concatenate([jnp.concatenate([zeros_block, scaled], axis=1), jnp.concatenate([-scaled.T, zeros_block], axis=1)], axis=0)
    iterate = jnp.eye(2 * half_width, dtype=jnp.float32) + generator
    for polar_index in range(POLAR_STEPS):
        product = jnp.dot(iterate, iterate.T, precision=HIGH)
        iterate = 1.5 * iterate - 0.5 * jnp.dot(product, iterate, precision=HIGH)
    return iterate

def advance(turned, flags):
    chosen = (flags == 1)[None, :, None]
    first_panel = turned[:, :, :P_SIZE]
    second_panel = turned[:, :, P_SIZE:]
    moving = jnp.where(chosen, second_panel, first_panel)
    staying = jnp.where(chosen, first_panel, second_panel)
    arriving = jnp.roll(moving, 1, axis=1)
    return jnp.concatenate([staying, arriving], axis=2)

def reference(activations, plan):
    matrix = activations
    vectors = jnp.eye(N, dtype=jnp.float32)
    for round_index in range(ROUNDS):
        stacked = matrix.reshape(M, PAIRS, 2 * P_SIZE)
        grams = jnp.einsum('mpa,mpb->pab', stacked, stacked, precision=HIGH)
        rotations = jax.vmap(rotation)(grams)
        turned = jnp.einsum('mpa,pab->mpb', stacked, rotations, precision=HIGH)
        vec_stack = vectors.reshape(N, PAIRS, 2 * P_SIZE)
        turned_vec = jnp.einsum('mpa,pab->mpb', vec_stack, rotations, precision=HIGH)
        matrix = advance(turned, plan[round_index]).reshape(M, N)
        vectors = advance(turned_vec, plan[round_index]).reshape(N, N)
    squares = lax.optimization_barrier(jnp.sum(matrix * matrix, axis=0))
    spread = jnp.sqrt(squares / M)
    return (matrix, vectors, spread)
```

```python
import functools

import jax
import jax.numpy as jnp
import numpy as np
from jax import lax
from jax.experimental import pallas as pl
from jax.experimental.pallas import tpu as pltpu
from jax.sharding import PartitionSpec as P

ROUNDS = 3
POLAR_STEPS = 3
TAIL = 8
VMEM = pl.BlockSpec(memory_space=pltpu.VMEM)
SMEM = pl.BlockSpec(memory_space=pltpu.SMEM)
PARAMS = pltpu.CompilerParams(vmem_limit_bytes=24 << 20)


def from_behind(block, axis, distance):
    count = lax.axis_size(axis)
    return lax.ppermute(block, axis, [((i - distance) % count, i) for i in range(count)])


def exchange(block, axis, bit):
    return lax.ppermute(block, axis, [(i, i ^ bit) for i in range(lax.axis_size(axis))])


def sum_rows(top, bottom):
    count = lax.axis_size("row")
    bits = [1 << k for k in range(count.bit_length() - 1)]
    assert 1 << len(bits) == count
    for k in range(len(bits)):
        top_in = exchange(top, "row", bits[k])
        bottom_in = exchange(bottom, "row", bits[(k + 1) % len(bits)])
        top, bottom = top + top_in, bottom + bottom_in
    return jnp.concatenate([top, bottom], axis=0)


def cut(value):
    high = value.astype(jnp.bfloat16)
    return high, (value - high.astype(jnp.float32)).astype(jnp.bfloat16)


def dot(left, right, dims=(((1,), (0,)), ((), ()))):
    one = lambda a, b: lax.dot_general(a, b, dims, preferred_element_type=jnp.float32)
    return one(left[0], right[0]) + (one(left[0], right[1]) + one(left[1], right[0]))


def polar_series():
    square, factor = [1.0, 1.0], [1.0]
    for _ in range(POLAR_STEPS):
        step = [-0.5 * c for c in square]
        step[0] += 1.5
        factor = np.convolve(factor, step)
        square = np.convolve(square, np.convolve(step, step))
    return [float(c) for c in factor[1:]]


def rotation_halves(pack_ref):
    half = pack_ref.shape[1]
    cut_row = half // 2
    tail = pack_ref[cut_row : cut_row + TAIL]
    cross = jnp.concatenate([pack_ref[:cut_row], pack_ref[cut_row + TAIL :]], axis=0)
    inverse = 1.0 / jnp.sqrt(tail + 1e-06)
    coupling = (cross * inverse.T[:, 0:1]) * inverse[1:2]
    strength = jnp.sqrt(jnp.sum(coupling * coupling))
    scaled = coupling * (1.0 / (1.0 + strength))
    b, bt = cut(scaled), cut(scaled.T)
    rows = lax.broadcasted_iota(jnp.int32, (half, half), 0)
    cols = lax.broadcasted_iota(jnp.int32, (half, half), 1)
    unit = (rows == cols).astype(jnp.float32)
    c = polar_series()
    x = cut(dot(b, bt))
    x2 = cut(dot(x, x))
    xb = dot(x, b)
    powers = [scaled, xb, dot(x2, b), dot(x2, cut(xb))]
    x4 = cut(dot(x2, x2))
    x8 = cut(dot(x4, x4))
    group = lambda k: sum(c[4 * k + j] * powers[j] for j in range(4))
    high = group(2) + c[12] * dot(x4, b)
    u = cut(group(0) + dot(x4, cut(group(1))) + dot(x8, cut(high)))
    first = unit + dot(u, bt)
    second = unit + dot(bt, u)
    over = scaled + dot(x, u)
    under = -over.T
    chosen = tail[2:3] > 0.5
    staying = jnp.where(chosen, first, over), jnp.where(chosen, under, second)
    moving = jnp.where(chosen, over, first), jnp.where(chosen, second, under)
    return staying, moving


def times(parts, matrix_refs):
    half = parts[0].shape[0]
    if len(matrix_refs) == 1:
        whole = cut(jnp.concatenate(parts, axis=0))
        return dot(cut(matrix_refs[0][...]), whole)
    return dot(cut(matrix_refs[0][...]), cut(parts[0])) + dot(
        cut(matrix_refs[1][...]), cut(parts[1])
    )


def store_gram(left, right, flag, top_ref, bottom_ref):
    cut_row = top_ref.shape[0] - TAIL
    cross = dot(cut(left), cut(right), (((0,), (0,)), ((), ())))
    top_ref[:cut_row] = cross[:cut_row]
    bottom_ref[...] = cross[cut_row:]
    top_ref[cut_row:] = jnp.zeros((TAIL, cross.shape[1]), jnp.float32)
    top_ref[cut_row : cut_row + 1] = jnp.sum(left * left, axis=0, keepdims=True)
    top_ref[cut_row + 1 : cut_row + 2] = jnp.sum(right * right, axis=0, keepdims=True)
    top_ref[cut_row + 2 : cut_row + 3] = jnp.full((1, cross.shape[1]), flag, jnp.float32)


def f32(*shape):
    return jax.ShapeDtypeStruct(shape, jnp.float32)


def gram_shapes(half):
    return [f32(half // 2 + TAIL, half), f32(half - half // 2, half)]


def cost(flops):
    return pl.CostEstimate(flops=int(flops), bytes_accessed=1 << 20, transcendentals=0)


def call(kernel, name, outs, specs, operands, flops, **extra):
    return pl.pallas_call(
        kernel,
        name=name,
        out_shape=outs,
        in_specs=specs,
        out_specs=[VMEM] * len(outs),
        compiler_params=PARAMS,
        cost_estimate=cost(flops),
        **extra,
    )(*operands)


def gram_kernel(matrix_ref, plan_ref, top_ref, bottom_ref):
    half = matrix_ref.shape[1] // 2
    flag = plan_ref[0, 0].astype(jnp.float32)
    store_gram(matrix_ref[:, :half], matrix_ref[:, half:], flag, top_ref, bottom_ref)


def own_kernel(count, pack_ref, *refs):
    matrix_refs, (staying_ref, panel_ref) = refs[:count], refs[count:]
    half = pack_ref.shape[1]
    staying, _ = rotation_halves(pack_ref)
    staying_ref[:half], staying_ref[half:] = staying
    panel_ref[...] = times(staying, matrix_refs)


def next_kernel(round_index, count, pack_ref, plan_ref, panel_ref, *refs):
    matrix_refs, outs = refs[:count], refs[count:]
    staying_ref, moving_ref, arrived_ref, top_ref, bottom_ref = outs
    half = pack_ref.shape[1]
    staying, moving = rotation_halves(pack_ref)
    arrived = times(moving, matrix_refs)
    arrived_ref[...] = arrived
    flag = plan_ref[round_index, 0].astype(jnp.float32)
    store_gram(panel_ref[...], arrived, flag, top_ref, bottom_ref)
    staying_ref[:half], staying_ref[half:] = staying
    moving_ref[:half], moving_ref[half:] = moving


def last_kernel(count, pack_ref, panel_ref, *refs):
    matrix_refs, (moving_ref, matrix_ref, sums_ref) = refs[:count], refs[count:]
    half = pack_ref.shape[1]
    _, moving = rotation_halves(pack_ref)
    panel = panel_ref[...]
    arrived = times(moving, matrix_refs)
    sums_ref[:, :half] = jnp.broadcast_to(jnp.sum(panel * panel, axis=0), (8, half))
    sums_ref[:, half:] = jnp.broadcast_to(jnp.sum(arrived * arrived, axis=0), (8, half))
    matrix_ref[:, :half] = panel
    matrix_ref[:, half:] = arrived
    moving_ref[:half], moving_ref[half:] = moving


def turn_kernel(count, staying_ref, *refs):
    matrix_refs, (panel_ref,) = refs[:count], refs[count:]
    half = staying_ref.shape[1]
    panel_ref[...] = times((staying_ref[:half], staying_ref[half:]), matrix_refs)


def holds(pair, rows_each):
    return lax.div(pair, rows_each) == lax.axis_index("row")


def middle_kernel(rows_each, s10, m11, s11, m12, s20, s21, m21, a0, b0, a1, b1, c1, d1, x1):
    half = s20.shape[1]
    pairs = lax.axis_size("col")
    top = lambda ref: cut(ref[:half])
    bottom = lambda ref: cut(ref[half:])
    own, near, side, far = (cut(ref[...]) for ref in (s10, m11, s11, m12))
    c_value = dot(side, top(m21))
    d_value = dot(far, bottom(m21))
    c1[...] = c_value
    d1[...] = d_value
    behind = lax.rem(lax.axis_index("col") + pairs - 1, pairs)
    x1[...] = jnp.where(holds(behind, rows_each), c_value, d_value)
    a0[...] = dot(own, top(s20))
    b0[...] = dot(near, bottom(s20))
    a1[...] = dot(side, top(s21))
    b1[...] = dot(far, bottom(s21))


def vectors_kernel(rows_each, a0, b0, a1, b1, c1, d1, x1, x2, s3, m3, out):
    half = s3.shape[1]
    pairs = lax.axis_size("col")
    pair = lax.axis_index("col")
    block = lax.axis_index("row") * rows_each + pl.program_id(0)
    behind = lax.rem(pair - block + pairs, pairs)
    zeros = jnp.zeros((out.shape[0], half), jnp.float32)
    top = lambda ref: cut(ref[:half])
    bottom = lambda ref: cut(ref[half:])
    whole = lambda ref: cut(ref[...])

    @pl.when(behind == 0)
    def _():
        out[:, :half] = dot(whole(a0), top(s3))
        out[:, half:] = zeros

    @pl.when(behind == 1)
    def _():
        out[:, :half] = dot(whole(b0), top(s3)) + dot(whole(c1), bottom(s3))
        out[:, half:] = dot(whole(a1), top(m3))

    @pl.when(behind == 2)
    def _():
        out[:, :half] = dot(whole(d1), bottom(s3))
        out[:, half:] = dot(whole(b1), top(m3)) + dot(whole(x1), bottom(m3))

    @pl.when(behind == 3)
    def _():
        two = lax.rem(pair + pairs - 2, pairs)
        far = jnp.where(lax.rem(two, rows_each) == 0, x1[...], x2[...])
        out[:, :half] = zeros
        out[:, half:] = dot(cut(far), bottom(m3))

    @pl.when(behind > 3)
    def _():
        out[:, :half] = zeros
        out[:, half:] = zeros


def per_device(activations, plan):
    rows, width = activations.shape
    half = width // 2
    row_count, pairs = lax.axis_size("row"), lax.axis_size("col")
    assert ROUNDS == 3 and pairs > ROUNDS and pairs % row_count == 0
    rows_each = pairs // row_count
    panel, turn = f32(rows, half), f32(width, half)
    cube = 6 * half**3
    turn_flops = 15 * cube + 6 * rows * width * half

    top, bottom = call(
        gram_kernel, "gram", gram_shapes(half), [VMEM, SMEM], (activations, plan), 2 * cube
    )
    own, near = (activations,), (from_behind(activations, "col", 1),)
    kept, sent, kept_near = [], [], []
    for round_index in range(ROUNDS):
        last = round_index + 1 == ROUNDS
        pack = sum_rows(top, bottom)
        pack_near = from_behind(pack, "col", 1)
        if round_index == 1:
            pack, far_turn = lax.optimization_barrier((pack, sent[0]))
            far_turn = from_behind(far_turn, "col", 1)
        if last:
            pack, c1, d1, x1 = lax.optimization_barrier((pack, c1, d1, x1))
            x2 = lax.ppermute(
                d1,
                "col",
                [(i, (i + 1) % pairs) for i in range(pairs) if (i - 1) % pairs % rows_each],
            )
            x1 = from_behind(x1, "col", 1)
        staying, still = call(
            functools.partial(own_kernel, len(own)),
            "own",
            [turn, panel],
            [VMEM] * (1 + len(own)),
            (pack, *own),
            turn_flops,
        )
        kept.append(staying)
        if last:
            moving, matrix, sums = call(
                functools.partial(last_kernel, len(near)),
                "last",
                [turn, f32(rows, width), f32(8, width)],
                [VMEM] * (2 + len(near)),
                (pack_near, still, *near),
                turn_flops,
            )
            sent.append(moving)
            break
        staying_near, moving, arrived, top, bottom = call(
            functools.partial(next_kernel, round_index + 1, len(near)),
            "next",
            [turn, turn, panel] + gram_shapes(half),
            [VMEM, SMEM, VMEM] + [VMEM] * len(near),
            (pack_near, plan, still, *near),
            turn_flops,
        )
        kept_near.append(staying_near)
        sent.append(moving)
        (still_near,) = call(
            functools.partial(turn_kernel, len(near)),
            "turn",
            [panel],
            [VMEM] * (1 + len(near)),
            (staying_near, *near),
            4 * cube,
        )
        own, near = (still, arrived), (still_near, from_behind(arrived, "col", 1))
        if round_index == 1:
            a0, b0, a1, b1, c1, d1, x1 = call(
                functools.partial(middle_kernel, rows_each),
                "middle",
                [turn] * 7,
                [VMEM] * 7,
                (kept[0], sent[0], kept_near[0], far_turn, kept[1], kept_near[1], sent[1]),
                12 * cube,
            )
    bits = [1 << k for k in range(row_count.bit_length() - 1)]
    for bit in bits:
        sums = sums + exchange(sums, "row", bit)
    spread = jnp.sqrt(sums[0] / (rows * row_count))
    vectors = pl.pallas_call(
        functools.partial(vectors_kernel, rows_each),
        name="vectors",
        grid=(rows_each,),
        out_shape=f32(rows_each * width, width),
        in_specs=[VMEM] * 10,
        out_specs=pl.BlockSpec((width, width), lambda i: (i, 0)),
        compiler_params=PARAMS,
        cost_estimate=cost(8 * cube),
    )(a0, b0, a1, b1, c1, d1, x1, x2, kept[2], sent[2])
    return (matrix, vectors, spread)


def solution(mesh):
    in_specs = (P("row", "col"), P(None, "col"))
    out_specs = (P("row", "col"), P("row", "col"), P("col"))
    return jax.shard_map(
        per_device, mesh=mesh, in_specs=in_specs, out_specs=out_specs, check_vma=False
    )
```

```python
import functools

import jax
import jax.numpy as jnp
import numpy as np
from jax import lax
from jax.experimental import pallas as pl
from jax.experimental.pallas import tpu as pltpu
from jax.sharding import PartitionSpec as P


ROUNDS = 3
POLAR_STEPS = 3
TAIL = 8
VMEM = pl.BlockSpec(memory_space=pltpu.VMEM)
PARAMS = pltpu.CompilerParams(vmem_limit_bytes=24 << 20)


def from_behind(block, axis, distance):
    count = lax.axis_size(axis)
    return lax.ppermute(block, axis, [((i - distance) % count, i) for i in range(count)])


def exchange(block, axis, mask):
    return lax.ppermute(block, axis, [(i, i ^ mask) for i in range(lax.axis_size(axis))])


def sum_rows(top, bottom, flag):
    count = lax.axis_size("row")
    bits = [1 << k for k in range(count.bit_length() - 1)]
    assert 1 << len(bits) == count
    for k in range(len(bits)):
        top_in = exchange(top, "row", bits[k])
        bottom_in = exchange(bottom, "row", bits[(k + 1) % len(bits)])
        top, bottom = top + top_in, bottom + bottom_in
    row = lax.broadcasted_iota(jnp.int32, top.shape, 0)
    top = jnp.where(row == top.shape[0] - TAIL + 2, flag.astype(jnp.float32), top)
    return jnp.concatenate([top, bottom], axis=0)


def cut(value):
    high = value.astype(jnp.bfloat16)
    return high, (value - high.astype(jnp.float32)).astype(jnp.bfloat16)


def dot(left, right, dims=(((1,), (0,)), ((), ()))):
    one = lambda a, b: lax.dot_general(a, b, dims, preferred_element_type=jnp.float32)
    return one(left[0], right[0]) + (one(left[0], right[1]) + one(left[1], right[0]))


def polar_series():
    square, factor = [1.0, 1.0], [1.0]
    for _ in range(POLAR_STEPS):
        step = [-0.5 * c for c in square]
        step[0] += 1.5
        factor = np.convolve(factor, step)
        square = np.convolve(square, np.convolve(step, step))
    return [float(c) for c in factor[1:]]


def rotation_halves(pack_ref):
    half = pack_ref.shape[1]
    cut_row = half // 2
    tail = pack_ref[cut_row : cut_row + TAIL]
    cross = jnp.concatenate([pack_ref[:cut_row], pack_ref[cut_row + TAIL :]], axis=0)
    inverse = 1.0 / jnp.sqrt(tail + 1e-06)
    coupling = (cross * inverse.T[:, 0:1]) * inverse[1:2]
    strength = jnp.sqrt(jnp.sum(coupling * coupling))
    scaled = coupling * (1.0 / (1.0 + strength))
    b, bt = cut(scaled), cut(scaled.T)
    rows = lax.broadcasted_iota(jnp.int32, (half, half), 0)
    cols = lax.broadcasted_iota(jnp.int32, (half, half), 1)
    unit = (rows == cols).astype(jnp.float32)
    c = polar_series()
    x = cut(dot(b, bt))
    x2 = cut(dot(x, x))
    xb = dot(x, b)
    powers = [scaled, xb, dot(x2, b), dot(x2, cut(xb))]
    x4 = cut(dot(x2, x2))
    x8 = cut(dot(x4, x4))
    group = lambda k: sum(c[4 * k + j] * powers[j] for j in range(4))
    high = group(2) + c[12] * dot(x4, b)
    u = cut(group(0) + dot(x4, cut(group(1))) + dot(x8, cut(high)))
    first = unit + dot(u, bt)
    second = unit + dot(bt, u)
    over = scaled + dot(x, u)
    under = -over.T
    chosen = tail[2:3] > 0.5
    staying = jnp.where(chosen, first, over), jnp.where(chosen, under, second)
    moving = jnp.where(chosen, over, first), jnp.where(chosen, second, under)
    return staying, moving


def times(parts, matrix_refs):
    if len(matrix_refs) == 1:
        whole = cut(jnp.concatenate(parts, axis=0))
        return dot(cut(matrix_refs[0][...]), whole)
    return dot(cut(matrix_refs[0][...]), cut(parts[0])) + dot(
        cut(matrix_refs[1][...]), cut(parts[1])
    )


def store_gram(left, right, top_ref, bottom_ref):
    cut_row = top_ref.shape[0] - TAIL
    cross = dot(cut(left), cut(right), (((0,), (0,)), ((), ())))
    top_ref[:cut_row] = cross[:cut_row]
    bottom_ref[...] = cross[cut_row:]
    top_ref[cut_row:] = jnp.zeros((TAIL, cross.shape[1]), jnp.float32)
    top_ref[cut_row : cut_row + 1] = jnp.sum(left * left, axis=0, keepdims=True)
    top_ref[cut_row + 1 : cut_row + 2] = jnp.sum(right * right, axis=0, keepdims=True)


def f32(*shape):
    return jax.ShapeDtypeStruct(shape, jnp.float32)


def gram_shapes(half):
    return [f32(half // 2 + TAIL, half), f32(half - half // 2, half)]


def cost(flops):
    return pl.CostEstimate(flops=int(flops), bytes_accessed=1 << 20, transcendentals=0)


def call(kernel, outs, specs, operands, flops, **extra):
    return pl.pallas_call(
        kernel,
        out_shape=outs,
        in_specs=specs,
        out_specs=[VMEM] * len(outs),
        compiler_params=PARAMS,
        cost_estimate=cost(flops),
        **extra,
    )(*operands)


def gram_kernel(matrix_ref, top_ref, bottom_ref):
    half = matrix_ref.shape[1] // 2
    store_gram(matrix_ref[:, :half], matrix_ref[:, half:], top_ref, bottom_ref)


def own_kernel(count, pack_ref, *refs):
    matrix_refs, (staying_ref, panel_ref) = refs[:count], refs[count:]
    half = pack_ref.shape[1]
    staying, _ = rotation_halves(pack_ref)
    staying_ref[:half], staying_ref[half:] = staying
    panel_ref[...] = times(staying, matrix_refs)


def next_kernel(count, pack_ref, panel_ref, *refs):
    matrix_refs, outs = refs[:count], refs[count:]
    staying_ref, moving_ref, arrived_ref, top_ref, bottom_ref = outs
    half = pack_ref.shape[1]
    staying, moving = rotation_halves(pack_ref)
    arrived = times(moving, matrix_refs)
    arrived_ref[...] = arrived
    store_gram(panel_ref[...], arrived, top_ref, bottom_ref)
    staying_ref[:half], staying_ref[half:] = staying
    moving_ref[:half], moving_ref[half:] = moving


def last_kernel(count, pack_ref, panel_ref, *refs):
    matrix_refs, (moving_ref, arrived_ref, sums_ref) = refs[:count], refs[count:]
    half = pack_ref.shape[1]
    _, moving = rotation_halves(pack_ref)
    panel = panel_ref[...]
    arrived = times(moving, matrix_refs)
    sums_ref[:, :half] = jnp.broadcast_to(jnp.sum(panel * panel, axis=0), (8, half))
    sums_ref[:, half:] = jnp.broadcast_to(jnp.sum(arrived * arrived, axis=0), (8, half))
    arrived_ref[...] = arrived
    moving_ref[:half], moving_ref[half:] = moving


def turn_kernel(count, staying_ref, *refs):
    matrix_refs, (panel_ref,) = refs[:count], refs[count:]
    half = staying_ref.shape[1]
    panel_ref[...] = times((staying_ref[:half], staying_ref[half:]), matrix_refs)


def holds(pair, rows_each):
    return lax.div(pair, rows_each) == lax.axis_index("row")


def middle_kernel(rows_each, s10, m11, s11, m12, s20, s21, m21, a0, b0, a1, b1, c1, d1, x1):
    half = s20.shape[1]
    pairs = lax.axis_size("col")
    top = lambda ref: cut(ref[:half])
    bottom = lambda ref: cut(ref[half:])
    own, near, side, far = (cut(ref[...]) for ref in (s10, m11, s11, m12))
    c_value = dot(side, top(m21))
    d_value = dot(far, bottom(m21))
    c1[...] = c_value
    d1[...] = d_value
    behind = lax.rem(lax.axis_index("col") + pairs - 1, pairs)
    x1[...] = jnp.where(holds(behind, rows_each), c_value, d_value)
    a0[...] = dot(own, top(s20))
    b0[...] = dot(near, bottom(s20))
    a1[...] = dot(side, top(s21))
    b1[...] = dot(far, bottom(s21))


def finish_kernel(rows_each, a0, b0, a1, b1, c1, d1, x1, x2, s3, m3, still, arrived, matrix, out):
    half = s3.shape[1]
    pairs = lax.axis_size("col")
    pair = lax.axis_index("col")
    block = lax.axis_index("row") * rows_each + pl.program_id(0)
    behind = lax.rem(pair - block + pairs, pairs)
    zeros = jnp.zeros((out.shape[0], half), jnp.float32)
    matrix[:, :half] = still[...]
    matrix[:, half:] = arrived[...]
    top = lambda ref: cut(ref[:half])
    bottom = lambda ref: cut(ref[half:])
    whole = lambda ref: cut(ref[...])

    @pl.when(behind == 0)
    def _():
        out[:, :half] = dot(whole(a0), top(s3))
        out[:, half:] = zeros

    @pl.when(behind == 1)
    def _():
        out[:, :half] = dot(whole(b0), top(s3)) + dot(whole(c1), bottom(s3))
        out[:, half:] = dot(whole(a1), top(m3))

    @pl.when(behind == 2)
    def _():
        out[:, :half] = dot(whole(d1), bottom(s3))
        out[:, half:] = dot(whole(b1), top(m3)) + dot(whole(x1), bottom(m3))

    @pl.when(behind == 3)
    def _():
        two = lax.rem(pair + pairs - 2, pairs)
        far = jnp.where(lax.rem(two, rows_each) == 0, x1[...], x2[...])
        out[:, :half] = zeros
        out[:, half:] = dot(cut(far), bottom(m3))

    @pl.when(behind > 3)
    def _():
        out[:, :half] = zeros
        out[:, half:] = zeros


def per_device(activations, plan):
    rows, width = activations.shape
    half = width // 2
    row_count, pairs = lax.axis_size("row"), lax.axis_size("col")
    assert ROUNDS == 3 and pairs > ROUNDS and pairs % row_count == 0
    rows_each = pairs // row_count
    panel, turn = f32(rows, half), f32(width, half)
    cube = 6 * half**3
    turn_flops = 15 * cube + 6 * rows * width * half

    top, bottom = call(gram_kernel, gram_shapes(half), [VMEM], (activations,), 2 * cube)
    near = (from_behind(activations, "col", 1),)
    own = (activations,)
    kept, sent, kept_near = [], [], []
    for round_index in range(ROUNDS):
        pack = sum_rows(top, bottom, plan[round_index, 0])
        pack_near = from_behind(pack, "col", 1)
        staying, still = call(
            functools.partial(own_kernel, len(own)),
            [turn, panel],
            [VMEM] * (1 + len(own)),
            (pack, *own),
            turn_flops,
        )
        kept.append(staying)
        if round_index + 1 == ROUNDS:
            break
        staying_near, moving, arrived, top, bottom = call(
            functools.partial(next_kernel, len(near)),
            [turn, turn, panel] + gram_shapes(half),
            [VMEM] * (2 + len(near)),
            (pack_near, still, *near),
            turn_flops,
        )
        kept_near.append(staying_near)
        sent.append(moving)
        arrived_near = from_behind(arrived, "col", 1)
        if round_index == 0:
            far_turn = from_behind(moving, "col", 1)
        else:
            a0, b0, a1, b1, c1, d1, x1 = call(
                functools.partial(middle_kernel, rows_each),
                [turn] * 7,
                [VMEM] * 7,
                (kept[0], sent[0], kept_near[0], far_turn, kept[1], staying_near, moving),
                12 * cube,
            )
            x1 = from_behind(x1, "col", 1)
            route = [(i, (i + 1) % pairs) for i in range(pairs)]
            x2 = lax.ppermute(d1, "col", [e for e in route if (e[0] - 1) % rows_each])
        (still_near,) = call(
            functools.partial(turn_kernel, len(near)),
            [panel],
            [VMEM] * (1 + len(near)),
            (staying_near, *near),
            4 * cube,
        )
        own, near = (still, arrived), (still_near, arrived_near)
    moving, arrived, sums = call(
        functools.partial(last_kernel, len(near)),
        [turn, panel, f32(8, width)],
        [VMEM] * (2 + len(near)),
        (pack_near, still, *near),
        turn_flops,
    )
    terms = [sums]
    for mask in range(1, row_count):
        terms.append(exchange(sums, "row", mask))
    matrix, vectors = pl.pallas_call(
        functools.partial(finish_kernel, rows_each),
        name="finish",
        grid=(rows_each,),
        out_shape=[f32(rows, width), f32(rows_each * width, width)],
        in_specs=[VMEM] * 10 + [pl.BlockSpec((rows // rows_each, half), lambda i: (i, 0))] * 2,
        out_specs=[
            pl.BlockSpec((rows // rows_each, width), lambda i: (i, 0)),
            pl.BlockSpec((width, width), lambda i: (i, 0)),
        ],
        compiler_params=PARAMS,
        cost_estimate=cost(8 * cube),
    )(a0, b0, a1, b1, c1, d1, x1, x2, kept[2], moving, still, arrived)
    totals = terms[0][0]
    for term in terms[1:]:
        totals = totals + term[0]
    spread = jnp.sqrt(totals / (rows * row_count))
    return (matrix, vectors, spread)


def solution(mesh):
    in_specs = (P("row", "col"), P(None, "col"))
    out_specs = (P("row", "col"), P("row", "col"), P("col"))
    return jax.shard_map(
        per_device, mesh=mesh, in_specs=in_specs, out_specs=out_specs, check_vma=False
    )
```

```python
import functools

import jax
import jax.numpy as jnp
import numpy as np
from jax import lax
from jax.experimental import pallas as pl
from jax.experimental.pallas import tpu as pltpu
from jax.sharding import PartitionSpec as P


ROUNDS = 3
POLAR_STEPS = 3
TAIL = 8
VMEM = pl.BlockSpec(memory_space=pltpu.VMEM)
PARAMS = pltpu.CompilerParams(vmem_limit_bytes=24 << 20)


def from_behind(block, axis, distance):
    count = lax.axis_size(axis)
    return lax.ppermute(block, axis, [((i - distance) % count, i) for i in range(count)])


def exchange(block, axis, mask):
    return lax.ppermute(block, axis, [(i, i ^ mask) for i in range(lax.axis_size(axis))])


def sum_rows(top, bottom, flag):
    count = lax.axis_size("row")
    bits = [1 << k for k in range(count.bit_length() - 1)]
    assert 1 << len(bits) == count
    for k in range(len(bits)):
        top_in = exchange(top, "row", bits[k])
        bottom_in = exchange(bottom, "row", bits[(k + 1) % len(bits)])
        top, bottom = top + top_in, bottom + bottom_in
    row = lax.broadcasted_iota(jnp.int32, top.shape, 0)
    top = jnp.where(row == top.shape[0] - TAIL + 2, flag, top)
    return top, bottom


def cut(value):
    high = value.astype(jnp.bfloat16)
    return high, (value - high.astype(jnp.float32)).astype(jnp.bfloat16)


def dot(left, right, dims=(((1,), (0,)), ((), ()))):
    one = lambda a, b: lax.dot_general(a, b, dims, preferred_element_type=jnp.float32)
    return one(left[0], right[0]) + (one(left[0], right[1]) + one(left[1], right[0]))


def polar_series():
    square, factor = [1.0, 1.0], [1.0]
    for _ in range(POLAR_STEPS):
        step = [-0.5 * c for c in square]
        step[0] += 1.5
        factor = np.convolve(factor, step)
        square = np.convolve(square, np.convolve(step, step))
    return [float(c) for c in factor[1:]]


def rotation_halves(top_ref, bottom_ref, wanted):
    half = top_ref.shape[1]
    cut_row = top_ref.shape[0] - TAIL
    tail = top_ref[cut_row:]
    cross = jnp.concatenate([top_ref[:cut_row], bottom_ref[...]], axis=0)
    inverse = 1.0 / jnp.sqrt(tail + 1e-06)
    coupling = (cross * inverse.T[:, 0:1]) * inverse[1:2]
    b, bt = cut(coupling), cut(coupling.T)
    factor = 1.0 / (1.0 + jnp.sqrt(jnp.sum(coupling * coupling)))
    rows = lax.broadcasted_iota(jnp.int32, (half, half), 0)
    cols = lax.broadcasted_iota(jnp.int32, (half, half), 1)
    unit = (rows == cols).astype(jnp.float32)
    c = polar_series()
    x = cut(dot(b, bt) * (factor * factor))
    x2 = cut(dot(x, x))
    xb = dot(x, b)
    powers = [coupling, xb, dot(x2, b), dot(x2, cut(xb))]
    x4 = cut(dot(x2, x2))
    x8 = cut(dot(x4, x4))
    group = lambda k: sum(c[4 * k + j] * powers[j] for j in range(4))
    high = group(2) + c[12] * dot(x4, b)
    series = group(0) + dot(x4, cut(group(1))) + dot(x8, cut(high))
    over = (coupling + dot(x, cut(series))) * factor
    under = -over.T
    u = cut(series * (factor * factor))
    chosen = tail[2:3] > 0.5
    if wanted == "both":
        first = unit + dot(u, bt)
        second = unit + dot(bt, u)
        staying = jnp.where(chosen, first, over), jnp.where(chosen, under, second)
        moving = jnp.where(chosen, over, first), jnp.where(chosen, second, under)
        return staying, moving
    if wanted == "moving":
        chosen = jnp.logical_not(chosen)
    pick = lambda yes, no: tuple(jnp.where(chosen, y, n) for y, n in zip(yes, no))
    block = unit + dot(pick(u, bt), pick(bt, u))
    return jnp.where(chosen, block, over), jnp.where(chosen, under, block)


def times(parts, matrix_refs):
    if len(matrix_refs) == 1:
        whole = cut(jnp.concatenate(parts, axis=0))
        return dot(cut(matrix_refs[0][...]), whole)
    return dot(cut(matrix_refs[0][...]), cut(parts[0])) + dot(
        cut(matrix_refs[1][...]), cut(parts[1])
    )


def store_gram(left, right, top_ref, bottom_ref):
    cut_row = top_ref.shape[0] - TAIL
    cross = dot(cut(left), cut(right), (((0,), (0,)), ((), ())))
    top_ref[:cut_row] = cross[:cut_row]
    bottom_ref[...] = cross[cut_row:]
    top_ref[cut_row:] = jnp.zeros((TAIL, cross.shape[1]), jnp.float32)
    top_ref[cut_row : cut_row + 1] = jnp.sum(left * left, axis=0, keepdims=True)
    top_ref[cut_row + 1 : cut_row + 2] = jnp.sum(right * right, axis=0, keepdims=True)


def f32(*shape):
    return jax.ShapeDtypeStruct(shape, jnp.float32)


def gram_shapes(half):
    return [f32(half // 2 + TAIL, half), f32(half - half // 2, half)]


def cost(flops):
    return pl.CostEstimate(flops=int(flops), bytes_accessed=1 << 20, transcendentals=0)


def call(kernel, outs, specs, operands, flops, **extra):
    return pl.pallas_call(
        kernel,
        out_shape=outs,
        in_specs=specs,
        out_specs=[VMEM] * len(outs),
        compiler_params=PARAMS,
        cost_estimate=cost(flops),
        **extra,
    )(*operands)


def gram_kernel(matrix_ref, top_ref, bottom_ref):
    half = matrix_ref.shape[1] // 2
    store_gram(matrix_ref[:, :half], matrix_ref[:, half:], top_ref, bottom_ref)


def own_kernel(count, gram_top, gram_bottom, *refs):
    matrix_refs, (staying_ref, panel_ref) = refs[:count], refs[count:]
    half = gram_top.shape[1]
    staying = rotation_halves(gram_top, gram_bottom, "staying")
    staying_ref[:half], staying_ref[half:] = staying
    panel_ref[...] = times(staying, matrix_refs)


def next_kernel(count, gram_top, gram_bottom, panel_ref, *refs):
    matrix_refs, outs = refs[:count], refs[count:]
    staying_ref, moving_ref, arrived_ref, top_ref, bottom_ref = outs
    half = gram_top.shape[1]
    staying, moving = rotation_halves(gram_top, gram_bottom, "both")
    arrived = times(moving, matrix_refs)
    arrived_ref[...] = arrived
    store_gram(panel_ref[...], arrived, top_ref, bottom_ref)
    staying_ref[:half], staying_ref[half:] = staying
    moving_ref[:half], moving_ref[half:] = moving


def last_kernel(count, gram_top, gram_bottom, panel_ref, *refs):
    matrix_refs, (moving_ref, arrived_ref, sums_ref) = refs[:count], refs[count:]
    half = gram_top.shape[1]
    moving = rotation_halves(gram_top, gram_bottom, "moving")
    panel = panel_ref[...]
    arrived = times(moving, matrix_refs)
    sums_ref[:, :half] = jnp.broadcast_to(jnp.sum(panel * panel, axis=0), (8, half))
    sums_ref[:, half:] = jnp.broadcast_to(jnp.sum(arrived * arrived, axis=0), (8, half))
    arrived_ref[...] = arrived
    moving_ref[:half], moving_ref[half:] = moving


def turn_kernel(count, staying_ref, *refs):
    matrix_refs, (panel_ref,) = refs[:count], refs[count:]
    half = staying_ref.shape[1]
    panel_ref[...] = times((staying_ref[:half], staying_ref[half:]), matrix_refs)


def holds(pair, rows_each):
    return lax.div(pair, rows_each) == lax.axis_index("row")


def middle_kernel(rows_each, s10, m11, s11, m12, s20, s21, m21, a0, b0, a1, b1, c1, d1, x1):
    half = s20.shape[1]
    pairs = lax.axis_size("col")
    top = lambda ref: cut(ref[:half])
    bottom = lambda ref: cut(ref[half:])
    own, near, side, far = (cut(ref[...]) for ref in (s10, m11, s11, m12))
    c_value = dot(side, top(m21))
    d_value = dot(far, bottom(m21))
    c1[...] = c_value
    d1[...] = d_value
    behind = lax.rem(lax.axis_index("col") + pairs - 1, pairs)
    x1[...] = jnp.where(holds(behind, rows_each), c_value, d_value)
    a0[...] = dot(own, top(s20))
    b0[...] = dot(near, bottom(s20))
    a1[...] = dot(side, top(s21))
    b1[...] = dot(far, bottom(s21))


def finish_kernel(rows_each, a0, b0, a1, b1, c1, d1, x1, x2, s3, m3, still, arrived, matrix, out):
    half = s3.shape[1]
    pairs = lax.axis_size("col")
    pair = lax.axis_index("col")
    block = lax.axis_index("row") * rows_each + pl.program_id(0)
    behind = lax.rem(pair - block + pairs, pairs)
    zeros = jnp.zeros((out.shape[0], half), jnp.float32)
    matrix[:, :half] = still[...]
    matrix[:, half:] = arrived[...]
    top = lambda ref: cut(ref[:half])
    bottom = lambda ref: cut(ref[half:])
    whole = lambda ref: cut(ref[...])

    @pl.when(behind == 0)
    def _():
        out[:, :half] = dot(whole(a0), top(s3))
        out[:, half:] = zeros

    @pl.when(behind == 1)
    def _():
        out[:, :half] = dot(whole(b0), top(s3)) + dot(whole(c1), bottom(s3))
        out[:, half:] = dot(whole(a1), top(m3))

    @pl.when(behind == 2)
    def _():
        out[:, :half] = dot(whole(d1), bottom(s3))
        out[:, half:] = dot(whole(b1), top(m3)) + dot(whole(x1), bottom(m3))

    @pl.when(behind == 3)
    def _():
        two = lax.rem(pair + pairs - 2, pairs)
        far = jnp.where(lax.rem(two, rows_each) == 0, x1[...], x2[...])
        out[:, :half] = zeros
        out[:, half:] = dot(cut(far), bottom(m3))

    @pl.when(behind > 3)
    def _():
        out[:, :half] = zeros
        out[:, half:] = zeros


def per_device(activations, plan):
    rows, width = activations.shape
    half = width // 2
    row_count, pairs = lax.axis_size("row"), lax.axis_size("col")
    assert ROUNDS == 3 and pairs > ROUNDS and pairs % row_count == 0
    rows_each = pairs // row_count
    panel, turn = f32(rows, half), f32(width, half)
    cube = 6 * half**3
    turn_flops = 15 * cube + 6 * rows * width * half

    top, bottom = call(gram_kernel, gram_shapes(half), [VMEM], (activations,), 2 * cube)
    near = (from_behind(activations, "col", 1),)
    own = (activations,)
    flags = [plan[round_index, 0].astype(jnp.float32) for round_index in range(ROUNDS)]
    kept, sent, kept_near = [], [], []
    for round_index in range(ROUNDS):
        pack = sum_rows(top, bottom, flags[round_index])
        top_near = from_behind(pack[0], "col", 1)
        bottom_near = from_behind(pack[1], "col", 1)
        pack_near = top_near, bottom_near
        staying, still = call(
            functools.partial(own_kernel, len(own)),
            [turn, panel],
            [VMEM] * (2 + len(own)),
            (*pack, *own),
            turn_flops,
        )
        kept.append(staying)
        if round_index + 1 == ROUNDS:
            break
        staying_near, moving, arrived, top, bottom = call(
            functools.partial(next_kernel, len(near)),
            [turn, turn, panel] + gram_shapes(half),
            [VMEM] * (3 + len(near)),
            (*pack_near, still, *near),
            turn_flops,
        )
        kept_near.append(staying_near)
        sent.append(moving)
        arrived_near = from_behind(arrived, "col", 1)
        if round_index == 0:
            far_turn = from_behind(moving, "col", 1)
        else:
            a0, b0, a1, b1, c1, d1, x1 = call(
                functools.partial(middle_kernel, rows_each),
                [turn] * 7,
                [VMEM] * 7,
                (kept[0], sent[0], kept_near[0], far_turn, kept[1], staying_near, moving),
                12 * cube,
            )
            route = [(i, (i + 1) % pairs) for i in range(pairs)]
            x2 = lax.ppermute(d1, "col", [e for e in route if (e[0] - 1) % rows_each])
            x1 = from_behind(x1, "col", 1)
        (still_near,) = call(
            functools.partial(turn_kernel, len(near)),
            [panel],
            [VMEM] * (1 + len(near)),
            (staying_near, *near),
            4 * cube,
        )
        own, near = (still, arrived), (still_near, arrived_near)
    moving, arrived, sums = call(
        functools.partial(last_kernel, len(near)),
        [turn, panel, f32(8, width)],
        [VMEM] * (3 + len(near)),
        (*pack_near, still, *near),
        turn_flops,
    )
    terms = [sums]
    for mask in range(1, row_count):
        terms.append(exchange(sums, "row", mask))
    matrix, vectors = pl.pallas_call(
        functools.partial(finish_kernel, rows_each),
        name="finish",
        grid=(rows_each,),
        out_shape=[f32(rows, width), f32(rows_each * width, width)],
        in_specs=[VMEM] * 10 + [pl.BlockSpec((rows // rows_each, half), lambda i: (i, 0))] * 2,
        out_specs=[
            pl.BlockSpec((rows // rows_each, width), lambda i: (i, 0)),
            pl.BlockSpec((width, width), lambda i: (i, 0)),
        ],
        compiler_params=PARAMS,
        cost_estimate=cost(8 * cube),
    )(a0, b0, a1, b1, c1, d1, x1, x2, kept[2], moving, still, arrived)
    totals = terms[0][0]
    for term in terms[1:]:
        totals = totals + term[0]
    spread = jnp.sqrt(totals / (rows * row_count))
    return (matrix, vectors, spread)


def solution(mesh):
    in_specs = (P("row", "col"), P(None, "col"))
    out_specs = (P("row", "col"), P("row", "col"), P("col"))
    return jax.shard_map(
        per_device, mesh=mesh, in_specs=in_specs, out_specs=out_specs, check_vma=False
    )
```

```python
import functools

import jax
import jax.numpy as jnp
import numpy as np
from jax import lax
from jax.experimental import pallas as pl
from jax.experimental.pallas import tpu as pltpu
from jax.sharding import PartitionSpec as P


ROUNDS = 3
POLAR_STEPS = 3
TAIL = 8
VMEM = pl.BlockSpec(memory_space=pltpu.VMEM)
PARAMS = pltpu.CompilerParams(vmem_limit_bytes=24 << 20)


def from_behind(block, axis, distance):
    count = lax.axis_size(axis)
    return lax.ppermute(block, axis, [((i - distance) % count, i) for i in range(count)])


def exchange(block, axis, mask):
    return lax.ppermute(block, axis, [(i, i ^ mask) for i in range(lax.axis_size(axis))])


def sum_rows(top, bottom, flag):
    count = lax.axis_size("row")
    bits = [1 << k for k in range(count.bit_length() - 1)]
    assert 1 << len(bits) == count
    for k in range(len(bits)):
        top_in = exchange(top, "row", bits[k])
        bottom_in = exchange(bottom, "row", bits[(k + 1) % len(bits)])
        top, bottom = top + top_in, bottom + bottom_in
    row = lax.broadcasted_iota(jnp.int32, top.shape, 0)
    top = jnp.where(row == top.shape[0] - TAIL + 2, flag, top)
    return top, bottom


def cut(value):
    high = value.astype(jnp.bfloat16)
    return high, (value - high.astype(jnp.float32)).astype(jnp.bfloat16)


def dot(left, right, dims=(((1,), (0,)), ((), ()))):
    one = lambda a, b: lax.dot_general(a, b, dims, preferred_element_type=jnp.float32)
    return one(left[0], right[0]) + (one(left[0], right[1]) + one(left[1], right[0]))


def exact_dot(left, right, dims=(((1,), (0,)), ((), ()))):
    return lax.dot_general(
        left, right, dims, precision=lax.Precision.HIGHEST, preferred_element_type=jnp.float32
    )


def polar_series():
    square, factor = [1.0, 1.0], [1.0]
    for _ in range(POLAR_STEPS):
        step = [-0.5 * c for c in square]
        step[0] += 1.5
        factor = np.convolve(factor, step)
        square = np.convolve(square, np.convolve(step, step))
    return [float(c) for c in factor[1:]]


def rotation_halves(top_ref, bottom_ref, wanted):
    half = top_ref.shape[1]
    cut_row = top_ref.shape[0] - TAIL
    tail = top_ref[cut_row:]
    cross = jnp.concatenate([top_ref[:cut_row], bottom_ref[...]], axis=0)
    inverse = 1.0 / jnp.sqrt(tail + 1e-06)
    coupling = (cross * inverse.T[:, 0:1]) * inverse[1:2]
    b, bt = cut(coupling), cut(coupling.T)
    factor = 1.0 / (1.0 + jnp.sqrt(jnp.sum(coupling * coupling)))
    rows = lax.broadcasted_iota(jnp.int32, (half, half), 0)
    cols = lax.broadcasted_iota(jnp.int32, (half, half), 1)
    unit = (rows == cols).astype(jnp.float32)
    c = polar_series()
    x = cut(dot(b, bt) * (factor * factor))
    x2 = cut(dot(x, x))
    xb = dot(x, b)
    powers = [coupling, xb, dot(x2, b), dot(x2, cut(xb))]
    x4 = cut(dot(x2, x2))
    x8 = cut(dot(x4, x4))
    group = lambda k: sum(c[4 * k + j] * powers[j] for j in range(4))
    high = group(2) + c[12] * dot(x4, b)
    series = group(0) + dot(x4, cut(group(1))) + dot(x8, cut(high))
    over = (coupling + dot(x, cut(series))) * factor
    under = -over.T
    u = cut(series * (factor * factor))
    chosen = tail[2:3] > 0.5
    if wanted == "both":
        first = unit + dot(u, bt)
        second = unit + dot(bt, u)
        staying = jnp.where(chosen, first, over), jnp.where(chosen, under, second)
        moving = jnp.where(chosen, over, first), jnp.where(chosen, second, under)
        return staying, moving
    if wanted == "moving":
        chosen = jnp.logical_not(chosen)
    pick = lambda yes, no: tuple(jnp.where(chosen, y, n) for y, n in zip(yes, no))
    block = unit + dot(pick(u, bt), pick(bt, u))
    return jnp.where(chosen, block, over), jnp.where(chosen, under, block)


def times(parts, matrix_refs):
    if len(matrix_refs) == 1:
        whole = jnp.concatenate(parts, axis=0)
        return exact_dot(matrix_refs[0][...], whole)
    return exact_dot(matrix_refs[0][...], parts[0]) + exact_dot(matrix_refs[1][...], parts[1])


def store_gram(left, right, top_ref, bottom_ref):
    cut_row = top_ref.shape[0] - TAIL
    cross = dot(cut(left), cut(right), (((0,), (0,)), ((), ())))
    top_ref[:cut_row] = cross[:cut_row]
    bottom_ref[...] = cross[cut_row:]
    top_ref[cut_row:] = jnp.zeros((TAIL, cross.shape[1]), jnp.float32)
    top_ref[cut_row : cut_row + 1] = jnp.sum(left * left, axis=0, keepdims=True)
    top_ref[cut_row + 1 : cut_row + 2] = jnp.sum(right * right, axis=0, keepdims=True)


def f32(*shape):
    return jax.ShapeDtypeStruct(shape, jnp.float32)


def gram_shapes(half):
    return [f32(half // 2 + TAIL, half), f32(half - half // 2, half)]


def cost(flops):
    return pl.CostEstimate(flops=int(flops), bytes_accessed=1 << 20, transcendentals=0)


def call(kernel, outs, specs, operands, flops, **extra):
    return pl.pallas_call(
        kernel,
        out_shape=outs,
        in_specs=specs,
        out_specs=[VMEM] * len(outs),
        compiler_params=PARAMS,
        cost_estimate=cost(flops),
        **extra,
    )(*operands)


def gram_kernel(matrix_ref, top_ref, bottom_ref):
    half = matrix_ref.shape[1] // 2
    store_gram(matrix_ref[:, :half], matrix_ref[:, half:], top_ref, bottom_ref)


def own_kernel(count, gram_top, gram_bottom, *refs):
    matrix_refs, (staying_ref, panel_ref) = refs[:count], refs[count:]
    half = gram_top.shape[1]
    staying = rotation_halves(gram_top, gram_bottom, "staying")
    staying_ref[:half], staying_ref[half:] = staying
    panel_ref[...] = times(staying, matrix_refs)


def next_kernel(count, gram_top, gram_bottom, panel_ref, *refs):
    matrix_refs, outs = refs[:count], refs[count:]
    staying_ref, moving_ref, arrived_ref, top_ref, bottom_ref = outs
    half = gram_top.shape[1]
    staying, moving = rotation_halves(gram_top, gram_bottom, "both")
    arrived = times(moving, matrix_refs)
    arrived_ref[...] = arrived
    store_gram(panel_ref[...], arrived, top_ref, bottom_ref)
    staying_ref[:half], staying_ref[half:] = staying
    moving_ref[:half], moving_ref[half:] = moving


def last_kernel(count, gram_top, gram_bottom, panel_ref, *refs):
    matrix_refs, (moving_ref, arrived_ref, sums_ref) = refs[:count], refs[count:]
    half = gram_top.shape[1]
    moving = rotation_halves(gram_top, gram_bottom, "moving")
    panel = panel_ref[...]
    arrived = times(moving, matrix_refs)
    sums_ref[:, :half] = jnp.broadcast_to(jnp.sum(panel * panel, axis=0), (8, half))
    sums_ref[:, half:] = jnp.broadcast_to(jnp.sum(arrived * arrived, axis=0), (8, half))
    arrived_ref[...] = arrived
    moving_ref[:half], moving_ref[half:] = moving


def turn_kernel(count, staying_ref, *refs):
    matrix_refs, (panel_ref,) = refs[:count], refs[count:]
    half = staying_ref.shape[1]
    panel_ref[...] = times((staying_ref[:half], staying_ref[half:]), matrix_refs)


def holds(pair, rows_each):
    return lax.div(pair, rows_each) == lax.axis_index("row")


def middle_kernel(rows_each, s10, m11, s11, m12, s20, s21, m21, a0, b0, a1, b1, c1, d1, x1):
    half = s20.shape[1]
    pairs = lax.axis_size("col")
    top = lambda ref: cut(ref[:half])
    bottom = lambda ref: cut(ref[half:])
    own, near, side, far = (cut(ref[...]) for ref in (s10, m11, s11, m12))
    c_value = dot(side, top(m21))
    d_value = dot(far, bottom(m21))
    c1[...] = c_value
    d1[...] = d_value
    behind = lax.rem(lax.axis_index("col") + pairs - 1, pairs)
    x1[...] = jnp.where(holds(behind, rows_each), c_value, d_value)
    a0[...] = dot(own, top(s20))
    b0[...] = dot(near, bottom(s20))
    a1[...] = dot(side, top(s21))
    b1[...] = dot(far, bottom(s21))


def finish_kernel(rows_each, a0, b0, a1, b1, c1, d1, x1, x2, s3, m3, still, arrived, matrix, out):
    half = s3.shape[1]
    pairs = lax.axis_size("col")
    pair = lax.axis_index("col")
    block = lax.axis_index("row") * rows_each + pl.program_id(0)
    behind = lax.rem(pair - block + pairs, pairs)
    zeros = jnp.zeros((out.shape[0], half), jnp.float32)
    matrix[:, :half] = still[...]
    matrix[:, half:] = arrived[...]
    top = lambda ref: cut(ref[:half])
    bottom = lambda ref: cut(ref[half:])
    whole = lambda ref: cut(ref[...])

    @pl.when(behind == 0)
    def _():
        out[:, :half] = dot(whole(a0), top(s3))
        out[:, half:] = zeros

    @pl.when(behind == 1)
    def _():
        out[:, :half] = dot(whole(b0), top(s3)) + dot(whole(c1), bottom(s3))
        out[:, half:] = dot(whole(a1), top(m3))

    @pl.when(behind == 2)
    def _():
        out[:, :half] = dot(whole(d1), bottom(s3))
        out[:, half:] = dot(whole(b1), top(m3)) + dot(whole(x1), bottom(m3))

    @pl.when(behind == 3)
    def _():
        two = lax.rem(pair + pairs - 2, pairs)
        far = jnp.where(lax.rem(two, rows_each) == 0, x1[...], x2[...])
        out[:, :half] = zeros
        out[:, half:] = dot(cut(far), bottom(m3))

    @pl.when(behind > 3)
    def _():
        out[:, :half] = zeros
        out[:, half:] = zeros


def per_device(activations, plan):
    rows, width = activations.shape
    half = width // 2
    row_count, pairs = lax.axis_size("row"), lax.axis_size("col")
    assert ROUNDS == 3 and pairs > ROUNDS and pairs % row_count == 0
    rows_each = pairs // row_count
    panel, turn = f32(rows, half), f32(width, half)
    cube = 6 * half**3
    turn_flops = 15 * cube + 6 * rows * width * half

    top, bottom = call(gram_kernel, gram_shapes(half), [VMEM], (activations,), 2 * cube)
    near = (from_behind(activations, "col", 1),)
    own = (activations,)
    flags = [plan[round_index, 0].astype(jnp.float32) for round_index in range(ROUNDS)]
    kept, sent, kept_near = [], [], []
    for round_index in range(ROUNDS):
        pack = sum_rows(top, bottom, flags[round_index])
        top_near = from_behind(pack[0], "col", 1)
        bottom_near = from_behind(pack[1], "col", 1)
        pack_near = top_near, bottom_near
        staying, still = call(
            functools.partial(own_kernel, len(own)),
            [turn, panel],
            [VMEM] * (2 + len(own)),
            (*pack, *own),
            turn_flops,
        )
        kept.append(staying)
        if round_index + 1 == ROUNDS:
            break
        staying_near, moving, arrived, top, bottom = call(
            functools.partial(next_kernel, len(near)),
            [turn, turn, panel] + gram_shapes(half),
            [VMEM] * (3 + len(near)),
            (*pack_near, still, *near),
            turn_flops,
        )
        kept_near.append(staying_near)
        sent.append(moving)
        arrived_near = from_behind(arrived, "col", 1)
        if round_index == 0:
            far_turn = from_behind(moving, "col", 1)
        else:
            a0, b0, a1, b1, c1, d1, x1 = call(
                functools.partial(middle_kernel, rows_each),
                [turn] * 7,
                [VMEM] * 7,
                (kept[0], sent[0], kept_near[0], far_turn, kept[1], staying_near, moving),
                12 * cube,
            )
            route = [(i, (i + 1) % pairs) for i in range(pairs)]
            x2 = lax.ppermute(d1, "col", [e for e in route if (e[0] - 1) % rows_each])
            x1 = from_behind(x1, "col", 1)
        (still_near,) = call(
            functools.partial(turn_kernel, len(near)),
            [panel],
            [VMEM] * (1 + len(near)),
            (staying_near, *near),
            4 * cube,
        )
        own, near = (still, arrived), (still_near, arrived_near)
    moving, arrived, sums = call(
        functools.partial(last_kernel, len(near)),
        [turn, panel, f32(8, width)],
        [VMEM] * (3 + len(near)),
        (*pack_near, still, *near),
        turn_flops,
    )
    terms = [sums]
    for mask in range(1, row_count):
        terms.append(exchange(sums, "row", mask))
    matrix, vectors = pl.pallas_call(
        functools.partial(finish_kernel, rows_each),
        name="finish",
        grid=(rows_each,),
        out_shape=[f32(rows, width), f32(rows_each * width, width)],
        in_specs=[VMEM] * 10 + [pl.BlockSpec((rows // rows_each, half), lambda i: (i, 0))] * 2,
        out_specs=[
            pl.BlockSpec((rows // rows_each, width), lambda i: (i, 0)),
            pl.BlockSpec((width, width), lambda i: (i, 0)),
        ],
        compiler_params=PARAMS,
        cost_estimate=cost(8 * cube),
    )(a0, b0, a1, b1, c1, d1, x1, x2, kept[2], moving, still, arrived)
    totals = terms[0][0]
    for term in terms[1:]:
        totals = totals + term[0]
    spread = jnp.sqrt(totals / (rows * row_count))
    return (matrix, vectors, spread)


def solution(mesh):
    in_specs = (P("row", "col"), P(None, "col"))
    out_specs = (P("row", "col"), P("row", "col"), P("col"))
    return jax.shard_map(
        per_device, mesh=mesh, in_specs=in_specs, out_specs=out_specs, check_vma=False
    )
```

```python
import functools

import jax
import jax.numpy as jnp
import numpy as np
from jax import lax
from jax.experimental import pallas as pl
from jax.experimental.pallas import tpu as pltpu
from jax.sharding import PartitionSpec as P


ROUNDS = 3
POLAR_STEPS = 3
TAIL = 8
VMEM = pl.BlockSpec(memory_space=pltpu.VMEM)
PARAMS = pltpu.CompilerParams(vmem_limit_bytes=24 << 20)


def from_behind(block, axis, distance):
    count = lax.axis_size(axis)
    return lax.ppermute(block, axis, [((i - distance) % count, i) for i in range(count)])


def exchange(block, axis, mask):
    return lax.ppermute(block, axis, [(i, i ^ mask) for i in range(lax.axis_size(axis))])


def sum_rows(top, bottom, flag):
    count = lax.axis_size("row")
    bits = [1 << k for k in range(count.bit_length() - 1)]
    assert 1 << len(bits) == count
    for k in range(len(bits)):
        top_in = exchange(top, "row", bits[k])
        bottom_in = exchange(bottom, "row", bits[(k + 1) % len(bits)])
        top, bottom = top + top_in, bottom + bottom_in
    row = lax.broadcasted_iota(jnp.int32, top.shape, 0)
    top = jnp.where(row == top.shape[0] - TAIL + 2, flag, top)
    return top, bottom


def cut(value):
    high = value.astype(jnp.bfloat16)
    return high, (value - high.astype(jnp.float32)).astype(jnp.bfloat16)


def dot(left, right, dims=(((1,), (0,)), ((), ()))):
    one = lambda a, b: lax.dot_general(a, b, dims, preferred_element_type=jnp.float32)
    return one(left[0], right[0]) + (one(left[0], right[1]) + one(left[1], right[0]))


def fine_dot(left, right):
    one = lambda x, y: jnp.dot(x, y, preferred_element_type=jnp.float32)
    high, low = cut(left)
    first, second = cut(right)
    third = (right - first.astype(jnp.float32) - second.astype(jnp.float32)).astype(jnp.bfloat16)
    return one(high, first) + (one(high, second) + one(low, first) + one(high, third))


def polar_series():
    square, factor = [1.0, 1.0], [1.0]
    for _ in range(POLAR_STEPS):
        step = [-0.5 * c for c in square]
        step[0] += 1.5
        factor = np.convolve(factor, step)
        square = np.convolve(square, np.convolve(step, step))
    return [float(c) for c in factor[1:]]


def rotation_halves(top_ref, bottom_ref, wanted):
    half = top_ref.shape[1]
    cut_row = top_ref.shape[0] - TAIL
    tail = top_ref[cut_row:]
    cross = jnp.concatenate([top_ref[:cut_row], bottom_ref[...]], axis=0)
    inverse = 1.0 / jnp.sqrt(tail + 1e-06)
    coupling = (cross * inverse.T[:, 0:1]) * inverse[1:2]
    b, bt = cut(coupling), cut(coupling.T)
    factor = 1.0 / (1.0 + jnp.sqrt(jnp.sum(coupling * coupling)))
    rows = lax.broadcasted_iota(jnp.int32, (half, half), 0)
    cols = lax.broadcasted_iota(jnp.int32, (half, half), 1)
    unit = (rows == cols).astype(jnp.float32)
    c = polar_series()
    x = cut(dot(b, bt) * (factor * factor))
    x2 = cut(dot(x, x))
    xb = dot(x, b)
    powers = [coupling, xb, dot(x2, b), dot(x2, cut(xb))]
    x4 = cut(dot(x2, x2))
    x8 = cut(dot(x4, x4))
    group = lambda k: sum(c[4 * k + j] * powers[j] for j in range(4))
    last = jnp.dot(x4[0], b[0], preferred_element_type=jnp.float32)
    high = group(2) + c[12] * last
    series = group(0) + dot(x4, cut(group(1))) + dot(x8, cut(high))
    over = (coupling + dot(x, cut(series))) * factor
    under = -over.T
    u = cut(series * (factor * factor))
    chosen = tail[2:3] > 0.5
    if wanted == "both":
        first = unit + dot(u, bt)
        second = unit + dot(bt, u)
        staying = jnp.where(chosen, first, over), jnp.where(chosen, under, second)
        moving = jnp.where(chosen, over, first), jnp.where(chosen, second, under)
        return staying, moving
    if wanted == "moving":
        chosen = jnp.logical_not(chosen)
    pick = lambda yes, no: tuple(jnp.where(chosen, y, n) for y, n in zip(yes, no))
    block = unit + dot(pick(u, bt), pick(bt, u))
    return jnp.where(chosen, block, over), jnp.where(chosen, under, block)


def times(parts, matrix_refs):
    if len(matrix_refs) == 1:
        whole = jnp.concatenate(parts, axis=0)
        return fine_dot(matrix_refs[0][...], whole)
    return fine_dot(matrix_refs[0][...], parts[0]) + fine_dot(matrix_refs[1][...], parts[1])


def store_gram(left, right, top_ref, bottom_ref):
    cut_row = top_ref.shape[0] - TAIL
    cross = dot(cut(left), cut(right), (((0,), (0,)), ((), ())))
    top_ref[:cut_row] = cross[:cut_row]
    bottom_ref[...] = cross[cut_row:]
    top_ref[cut_row:] = jnp.zeros((TAIL, cross.shape[1]), jnp.float32)
    top_ref[cut_row : cut_row + 1] = jnp.sum(left * left, axis=0, keepdims=True)
    top_ref[cut_row + 1 : cut_row + 2] = jnp.sum(right * right, axis=0, keepdims=True)


def f32(*shape):
    return jax.ShapeDtypeStruct(shape, jnp.float32)


def gram_shapes(half):
    return [f32(half // 2 + TAIL, half), f32(half - half // 2, half)]


def cost(flops):
    return pl.CostEstimate(flops=int(flops), bytes_accessed=1 << 20, transcendentals=0)


def call(kernel, outs, specs, operands, flops, **extra):
    return pl.pallas_call(
        kernel,
        out_shape=outs,
        in_specs=specs,
        out_specs=[VMEM] * len(outs),
        compiler_params=PARAMS,
        cost_estimate=cost(flops),
        **extra,
    )(*operands)


def gram_kernel(matrix_ref, top_ref, bottom_ref):
    half = matrix_ref.shape[1] // 2
    store_gram(matrix_ref[:, :half], matrix_ref[:, half:], top_ref, bottom_ref)


def own_kernel(count, gram_top, gram_bottom, *refs):
    matrix_refs, (staying_ref, panel_ref) = refs[:count], refs[count:]
    half = gram_top.shape[1]
    staying = rotation_halves(gram_top, gram_bottom, "staying")
    staying_ref[:half], staying_ref[half:] = staying
    panel_ref[...] = times(staying, matrix_refs)


def next_kernel(count, gram_top, gram_bottom, panel_ref, *refs):
    matrix_refs, outs = refs[:count], refs[count:]
    staying_ref, moving_ref, arrived_ref, top_ref, bottom_ref = outs
    half = gram_top.shape[1]
    staying, moving = rotation_halves(gram_top, gram_bottom, "both")
    arrived = times(moving, matrix_refs)
    arrived_ref[...] = arrived
    store_gram(panel_ref[...], arrived, top_ref, bottom_ref)
    staying_ref[:half], staying_ref[half:] = staying
    moving_ref[:half], moving_ref[half:] = moving


def last_kernel(count, gram_top, gram_bottom, panel_ref, *refs):
    matrix_refs, (moving_ref, arrived_ref, sums_ref) = refs[:count], refs[count:]
    half = gram_top.shape[1]
    moving = rotation_halves(gram_top, gram_bottom, "moving")
    panel = panel_ref[...]
    arrived = times(moving, matrix_refs)
    sums_ref[:, :half] = jnp.broadcast_to(jnp.sum(panel * panel, axis=0), (8, half))
    sums_ref[:, half:] = jnp.broadcast_to(jnp.sum(arrived * arrived, axis=0), (8, half))
    arrived_ref[...] = arrived
    moving_ref[:half], moving_ref[half:] = moving


def turn_kernel(count, staying_ref, *refs):
    matrix_refs, (panel_ref,) = refs[:count], refs[count:]
    half = staying_ref.shape[1]
    panel_ref[...] = times((staying_ref[:half], staying_ref[half:]), matrix_refs)


def holds(pair, rows_each):
    return lax.div(pair, rows_each) == lax.axis_index("row")


def middle_kernel(rows_each, s10, m11, s11, m12, s20, s21, m21, a0, b0, a1, b1, c1, d1, x1):
    half = s20.shape[1]
    pairs = lax.axis_size("col")
    top = lambda ref: cut(ref[:half])
    bottom = lambda ref: cut(ref[half:])
    own, near, side, far = (cut(ref[...]) for ref in (s10, m11, s11, m12))
    c_value = dot(side, top(m21))
    d_value = dot(far, bottom(m21))
    c1[...] = c_value
    d1[...] = d_value
    behind = lax.rem(lax.axis_index("col") + pairs - 1, pairs)
    x1[...] = jnp.where(holds(behind, rows_each), c_value, d_value)
    a0[...] = dot(own, top(s20))
    b0[...] = dot(near, bottom(s20))
    a1[...] = dot(side, top(s21))
    b1[...] = dot(far, bottom(s21))


def finish_kernel(rows_each, a0, b0, a1, b1, c1, d1, x1, x2, s3, m3, still, arrived, matrix, out):
    half = s3.shape[1]
    pairs = lax.axis_size("col")
    pair = lax.axis_index("col")
    block = lax.axis_index("row") * rows_each + pl.program_id(0)
    behind = lax.rem(pair - block + pairs, pairs)
    zeros = jnp.zeros((out.shape[0], half), jnp.float32)
    matrix[:, :half] = still[...]
    matrix[:, half:] = arrived[...]
    top = lambda ref: cut(ref[:half])
    bottom = lambda ref: cut(ref[half:])
    whole = lambda ref: cut(ref[...])

    @pl.when(behind == 0)
    def _():
        out[:, :half] = dot(whole(a0), top(s3))
        out[:, half:] = zeros

    @pl.when(behind == 1)
    def _():
        out[:, :half] = dot(whole(b0), top(s3)) + dot(whole(c1), bottom(s3))
        out[:, half:] = dot(whole(a1), top(m3))

    @pl.when(behind == 2)
    def _():
        out[:, :half] = dot(whole(d1), bottom(s3))
        out[:, half:] = dot(whole(b1), top(m3)) + dot(whole(x1), bottom(m3))

    @pl.when(behind == 3)
    def _():
        two = lax.rem(pair + pairs - 2, pairs)
        far = jnp.where(lax.rem(two, rows_each) == 0, x1[...], x2[...])
        out[:, :half] = zeros
        out[:, half:] = dot(cut(far), bottom(m3))

    @pl.when(behind > 3)
    def _():
        out[:, :half] = zeros
        out[:, half:] = zeros


def per_device(activations, plan):
    rows, width = activations.shape
    half = width // 2
    row_count, pairs = lax.axis_size("row"), lax.axis_size("col")
    assert ROUNDS == 3 and pairs > ROUNDS and pairs % row_count == 0
    rows_each = pairs // row_count
    panel, turn = f32(rows, half), f32(width, half)
    cube = 6 * half**3
    turn_flops = 15 * cube + 6 * rows * width * half

    top, bottom = call(gram_kernel, gram_shapes(half), [VMEM], (activations,), 2 * cube)
    near = (from_behind(activations, "col", 1),)
    own = (activations,)
    flags = [plan[round_index, 0].astype(jnp.float32) for round_index in range(ROUNDS)]
    kept, sent, kept_near = [], [], []
    for round_index in range(ROUNDS):
        pack = sum_rows(top, bottom, flags[round_index])
        top_near = from_behind(pack[0], "col", 1)
        bottom_near = from_behind(pack[1], "col", 1)
        pack_near = top_near, bottom_near
        staying, still = call(
            functools.partial(own_kernel, len(own)),
            [turn, panel],
            [VMEM] * (2 + len(own)),
            (*pack, *own),
            turn_flops,
        )
        kept.append(staying)
        if round_index + 1 == ROUNDS:
            break
        staying_near, moving, arrived, top, bottom = call(
            functools.partial(next_kernel, len(near)),
            [turn, turn, panel] + gram_shapes(half),
            [VMEM] * (3 + len(near)),
            (*pack_near, still, *near),
            turn_flops,
        )
        kept_near.append(staying_near)
        sent.append(moving)
        arrived_near = from_behind(arrived, "col", 1)
        if round_index == 0:
            far_turn = from_behind(moving, "col", 1)
        else:
            a0, b0, a1, b1, c1, d1, x1 = call(
                functools.partial(middle_kernel, rows_each),
                [turn] * 7,
                [VMEM] * 7,
                (kept[0], sent[0], kept_near[0], far_turn, kept[1], staying_near, moving),
                12 * cube,
            )
            route = [(i, (i + 1) % pairs) for i in range(pairs)]
            x2 = lax.ppermute(d1, "col", [e for e in route if (e[0] - 1) % rows_each])
            x1 = from_behind(x1, "col", 1)
        (still_near,) = call(
            functools.partial(turn_kernel, len(near)),
            [panel],
            [VMEM] * (1 + len(near)),
            (staying_near, *near),
            4 * cube,
        )
        own, near = (still, arrived), (still_near, arrived_near)
    moving, arrived, sums = call(
        functools.partial(last_kernel, len(near)),
        [turn, panel, f32(8, width)],
        [VMEM] * (3 + len(near)),
        (*pack_near, still, *near),
        turn_flops,
    )
    terms = [sums]
    for mask in range(1, row_count):
        terms.append(exchange(sums, "row", mask))
    matrix, vectors = pl.pallas_call(
        functools.partial(finish_kernel, rows_each),
        name="finish",
        grid=(rows_each,),
        out_shape=[f32(rows, width), f32(rows_each * width, width)],
        in_specs=[VMEM] * 10 + [pl.BlockSpec((rows // rows_each, half), lambda i: (i, 0))] * 2,
        out_specs=[
            pl.BlockSpec((rows // rows_each, width), lambda i: (i, 0)),
            pl.BlockSpec((width, width), lambda i: (i, 0)),
        ],
        compiler_params=PARAMS,
        cost_estimate=cost(8 * cube),
    )(a0, b0, a1, b1, c1, d1, x1, x2, kept[2], moving, still, arrived)
    totals = terms[0][0]
    for term in terms[1:]:
        totals = totals + term[0]
    spread = jnp.sqrt(totals / (rows * row_count))
    return (matrix, vectors, spread)


def solution(mesh):
    in_specs = (P("row", "col"), P(None, "col"))
    out_specs = (P("row", "col"), P("row", "col"), P("col"))
    return jax.shard_map(
        per_device, mesh=mesh, in_specs=in_specs, out_specs=out_specs, check_vma=False
    )
```
